32 devices in a mesh: gx: 2 (over x), gy: 4 (over y, core), ha: 4 (over z).
Axes of the slice: x: 2, y: 2, z: 4, core: 2. Of those that a mesh axis runs over, the one named last changes fastest.
Arguments:
- global_state: float32 [8, 60, 16, 16], P(None, 'ha', 'gx', 'gy'), may hold values from -6 to 6
- crm_state: float32 [8, 60, 16, 1024], P(None, 'ha', 'gx', 'gy'), may hold values from -6 to 6
- mixing: float32 [8, 8], replicated, may hold values from -2 to 2
- substeps: int32 [16, 16], P('gx', 'gy'), may hold values from 1 to 8
- assignment: int32 [16, 16], P('gx', 'gy'), may hold values from 0 to 31, as said below
Outputs:
- new_global: float32 [8, 60, 16, 16], P(None, 'ha', 'gx', 'gy')
- new_crm: float32 [8, 60, 16384], P(None, None, ('gx', 'gy', 'ha'))
The draws below stay inside these ranges and needn't reach their ends.
Inputs may be any that keep to these rules, and one draw needn't show every extreme that they name: `assignment`: within each tile of 8 x 4 columns every value 0 .. 31 appears once; value // 8 is the helper index, value % 8 the slot on that helper.
All inputs are finite; a program needn't handle non-finite values.
Results may differ from the reference program's by a relative error of at most 0.0003.
Values sent between devices are 32-bit elements; how exact they have to be, the bound alone decides.
A program may use at most 64 MiB of HBM per device.

```python
import jax
import jax.numpy as jnp
from jax import lax

CX = 8
CY = 4
GF = 8
CF = 8
LEV = 60
CC = 64
MAXSUB = 8
GSUB = 4
NXG = 16
NYG = 16
SLOTS = 8
N_GX = 2
N_GY = 4


def joint_draw(key):
    base = jax.random.fold_in(key, 31)
    counts = jax.random.randint(jax.random.fold_in(base, 1), (NXG, NYG), 1, 9)
    tiles_x = NXG // CX
    tiles_y = NYG // CY
    columns = CX * CY
    helpers = columns // SLOTS
    tiled = counts.reshape(tiles_x, CX, tiles_y, CY).transpose(0, 2, 1, 3).reshape(tiles_x * tiles_y, columns)
    noise = jax.random.randint(jax.random.fold_in(base, 2), tiled.shape, 0, 64)
    score = (tiled * 64 + noise) * columns + jnp.arange(columns, dtype=jnp.int32)[None, :]
    order = jnp.argsort(-score, axis=1, stable=True)
    ranking = jnp.argsort(order, axis=1, stable=True)
    lanes = ranking % helpers
    rounds = ranking // helpers
    helper = jnp.where(rounds % 2 == 0, lanes, helpers - 1 - lanes)
    values = helper * SLOTS + rounds
    placed = values.reshape(tiles_x, tiles_y, CX, CY).transpose(0, 2, 1, 3).reshape(NXG, NYG)
    return (counts.astype(jnp.int32), placed.astype(jnp.int32))


def draw_substeps(key, part):
    return joint_draw(key)[0]


def draw_assignment(key, part):
    return joint_draw(key)[1]


def steps_of(key, dims, shards, smallest, largest):
    gain = 1.0
    for position, blocks in shards:
        steps = jax.random.uniform(jax.random.fold_in(jax.random.fold_in(key, 6), position), (blocks,), jnp.float32, smallest / len(shards), largest / len(shards))
        gain = gain * jnp.repeat(jnp.exp(steps), dims[position] // blocks).reshape((-1,) + (1,) * (len(dims) - 1 - position))
    return gain


def gaussian(own_key, extent, width, most, shards=(), held_as=jnp.bfloat16):
    drawn = jax.random.normal(own_key, extent, jnp.float32) * width
    if len(shards) > 0:
        drawn = steps_of(own_key, extent, shards, -0.22, 0.18) * drawn
    return jnp.clip(drawn, min=-most, max=most).astype(held_as)


def setup_inputs(seed: int = 0) -> dict:
    seeds = jax.random.split(jax.random.key(seed), 6)
    global_state = gaussian(seeds[0], (GF, LEV, NXG, NYG), 1.0, 6.0, ((1, 4), (2, 2), (3, 4)), jnp.float32)
    crm_state = gaussian(seeds[1], (CF, LEV, NXG, NYG * CC), 1.0, 6.0, ((1, 4), (2, 2), (3, 4)), jnp.float32)
    mixing = gaussian(seeds[2], (CF, CF), CF ** -0.5, 2.0, (), jnp.float32)
    substeps = draw_substeps(jax.random.fold_in(seeds[5], 71), 0)
    assignment = draw_assignment(jax.random.fold_in(seeds[5], 71), 0)
    return dict(global_state=global_state, crm_state=crm_state, mixing=mixing, substeps=substeps, assignment=assignment)


HIGH = lax.Precision.HIGHEST


def global_operator(field):
    east = jnp.roll(field, -1, axis=2)
    west = jnp.roll(field, 1, axis=2)
    north = jnp.roll(field, -1, axis=3)
    south = jnp.roll(field, 1, axis=3)
    return 0.2 * (east + west + north + south - 4.0 * field) - 0.15 * (east - west) - 0.15 * (north - south)


def crm_update(state, pushed, mixing):
    lateral = jnp.roll(state, 1, axis=3) + jnp.roll(state, -1, axis=3) - 2.0 * state
    upper = jnp.concatenate([state[:, :1], state[:, :-1]], axis=1)
    lower = jnp.concatenate([state[:, 1:], state[:, -1:]], axis=1)
    coupling = jnp.einsum('gf,flsc->glsc', mixing, jnp.tanh(state), precision=HIGH)
    return state + 0.1 * (1.0 * lateral + 0.5 * (upper + lower - 2.0 * state) + pushed + coupling)


def to_tiles(array, lead):
    shaped = array.reshape(array.shape[:lead] + (N_GX, CX, N_GY, CY))
    moved = jnp.moveaxis(shaped, (lead, lead + 2), (0, 1))
    return moved.reshape((N_GX * N_GY,) + array.shape[:lead] + (CX * CY,))


def from_tiles(array, lead):
    inner = array.shape[1:1 + lead]
    shaped = array.reshape((N_GX, N_GY) + inner + (CX, CY))
    moved = jnp.moveaxis(shaped, (0, 1), (lead, lead + 2))
    return moved.reshape(inner + (CX * N_GX, CY * N_GY))


def reference(global_state, crm_state, mixing, substeps, assignment):
    current = global_state
    for substep in range(GSUB):
        current = current + 0.5 * global_operator(current)
    forcing = (current - global_state) / (0.5 * GSUB)
    columns = CX * CY
    shaped = crm_state.reshape(CF, LEV, N_GX, CX, N_GY, CY, CC)
    shaped = jnp.moveaxis(shaped, (2, 4), (0, 1))
    state_tiles = shaped.reshape(N_GX * N_GY, CF, LEV, columns, CC)
    forcing_tiles = to_tiles(forcing, 2)
    count_tiles = to_tiles(substeps, 0)
    assign_tiles = to_tiles(assignment, 0)

    def per_tile(inputs):
        states, pushes, counts, assigned = inputs
        onehot = (assigned[:, None] == jnp.arange(columns, dtype=jnp.int32)[None, :]).astype(jnp.float32)
        slotted = jnp.einsum('flxc,xj->fljc', states, onehot, precision=HIGH)
        pushed = jnp.einsum('glx,xj->glj', pushes, onehot, precision=HIGH)[:, :, :, None]
        slot_counts = jnp.dot(counts.astype(jnp.float32), onehot, precision=HIGH).astype(jnp.int32)

        def one_step(index, state):
            updated = crm_update(state, pushed, mixing)
            return jnp.where((index < slot_counts)[:, None], updated, state)

        final = lax.fori_loop(0, MAXSUB, one_step, slotted)
        tendency = jnp.mean(final - slotted, axis=3)
        placed = jnp.einsum('flj,xj->flx', tendency, onehot, precision=HIGH)
        return final, placed

    finals, placed = lax.map(per_tile, (state_tiles, forcing_tiles, count_tiles, assign_tiles))
    new_crm = jnp.moveaxis(finals, 0, 2).reshape((CF, LEV, N_GX * N_GY * columns * CC))
    new_global = current + from_tiles(placed, 2)
    return new_global, new_crm
```

```python
import functools

import jax
import jax.numpy as jnp
from jax import lax
from jax.experimental import pallas as pl
from jax.experimental.pallas import tpu as pltpu
from jax.sharding import PartitionSpec as P

MAXSUB = 8
GSUB = 4
LANES = 128
MESH = pl.DeviceIdType.MESH
HIGH = lax.Precision.HIGHEST
F32 = jnp.float32
I32 = jnp.int32


def lane_iota(shape):
    return lax.broadcasted_iota(I32, shape, len(shape) - 1)


def slot_kernel(dims, assign_ref, steps_ref, low_ref, high_ref, slots_ref, table_ref):
    fields, levels, tile_x, tile_y, width, helpers, pairs = dims
    columns = tile_x * tile_y
    for x in range(tile_x):
        for y in range(tile_y):
            v = assign_ref[x, y]
            table_ref[v] = x * tile_y + y
            table_ref[columns + v] = steps_ref[x, y]
    lane = lane_iota((fields, LANES))
    even = lax.rem(lane, 2) == 0
    half = lax.div(lane, 2)

    def one_pair(q, carry):
        ca = table_ref[2 * q]
        cb = table_ref[2 * q + 1]
        xa, ya = lax.div(ca, tile_y), lax.rem(ca, tile_y)
        xb, yb = lax.div(cb, tile_y), lax.rem(cb, tile_y)
        ia = half + lax.rem(ya, 2) * width
        ib = half + lax.rem(yb, 2) * width
        ta, tb = ya < 2, yb < 2
        for l in range(levels):
            rows_a = pl.ds(l * tile_x + xa, fields, stride=levels * tile_x)
            rows_b = pl.ds(l * tile_x + xb, fields, stride=levels * tile_x)
            a = jnp.where(ta, low_ref[rows_a, :], high_ref[rows_a, :])
            b = jnp.where(tb, low_ref[rows_b, :], high_ref[rows_b, :])
            a = jnp.take_along_axis(a, ia, axis=1)
            b = jnp.take_along_axis(b, ib, axis=1)
            slots_ref[q * levels + l] = jnp.where(even, a, b)
        return carry

    lax.fori_loop(0, helpers * pairs, one_pair, 0)


def order_kernel(dims, in_ref, out_ref):
    fields, levels_all, width = dims
    for f in range(fields):
        for l in range(0, levels_all, 8):
            rows = min(8, levels_all - l)
            lane = lane_iota((rows, LANES))
            index = 2 * lax.rem(lane, width) + lax.div(lane, width)
            v = in_ref[pl.ds(l * fields + f, rows, stride=fields), :]
            out_ref[f, l:l + rows, :] = jnp.take_along_axis(v, index, axis=1)


def pair_sum(v):
    shift = 2
    while shift < LANES:
        v = v + pltpu.roll(v, shift, 1)
        shift *= 2
    return v


def exchange_kernel(
    dims, sizes, assign_ref, table_ref, slots_ref, g_ref, mixing_ref, crm_ref, newg_ref,
    state, push, ext, g4, fcol, fsend, frecv, tsend, trecv, mask,
    halo_send, halo_recv, crm_send, crm_recv, f_send, f_recv, t_send, t_recv,
):
    fields, levels, tile_x, tile_y, width, helpers, pairs = dims
    n_gx, n_gy = sizes
    columns = tile_x * tile_y
    levels_all = levels * helpers
    slots = 2 * pairs
    span = LANES // tile_y
    h = GSUB
    gx, gy, ha = lax.axis_index("gx"), lax.axis_index("gy"), lax.axis_index("ha")

    offsets = [(dx, dy) for dx in (0, 1, -1) for dy in (0, 1, -1) if (dx, dy) != (0, 0)]

    def tile_at(dx, dy):
        return {"gx": lax.rem(gx + dx + n_gx, n_gx), "gy": lax.rem(gy + dy + n_gy, n_gy)}

    peers = [lax.rem(ha + i, helpers) for i in range(1, helpers)]
    barrier = pltpu.get_barrier_semaphore()
    for dx, dy in offsets:
        pl.semaphore_signal(barrier, inc=1, device_id=tile_at(dx, dy), device_id_type=MESH)
    for peer in peers:
        pl.semaphore_signal(barrier, inc=1, device_id={"ha": peer}, device_id_type=MESH)
    pl.semaphore_wait(barrier, len(offsets) + len(peers))

    halos = []
    for o, (dx, dy) in enumerate(offsets):
        if dx == 0:
            src, dst = g_ref, ext.at[1 - dy, pl.ds(h, tile_x)]
        elif dx == 1:
            src, dst = g_ref.at[pl.ds(tile_x - h, h)], ext.at[1 - dy, pl.ds(0, h)]
        else:
            src, dst = g_ref.at[pl.ds(0, h)], ext.at[1 - dy, pl.ds(tile_x + h, h)]
        halos.append(pltpu.make_async_remote_copy(
            src_ref=src, dst_ref=dst, send_sem=halo_send.at[o], recv_sem=halo_recv.at[o],
            device_id=tile_at(dx, dy), device_id_type=MESH))
        halos[-1].start()
    moves = []
    for p in range(pairs):
        row = []
        for i, peer in enumerate(peers):
            row.append(pltpu.make_async_remote_copy(
                src_ref=slots_ref.at[pl.ds((peer * pairs + p) * levels, levels)],
                dst_ref=state.at[p, pl.ds(ha * levels, levels)],
                send_sem=crm_send.at[p, i], recv_sem=crm_recv.at[p, i],
                device_id={"ha": peer}, device_id_type=MESH))
            row[-1].start()
        moves.append(row)

    for p in range(pairs):
        for l in range(levels):
            state[p, ha * levels + l] = slots_ref[(ha * pairs + p) * levels + l]
    ext[1, h:h + tile_x] = g_ref[...]
    lane = lane_iota((fields, LANES))
    lane3 = lane_iota((1, 1, LANES))
    for copy in halos:
        copy.wait_recv()
    tiles = [ext[t] for t in range(3)]
    for _ in range(GSUB):
        up = [pltpu.roll(t, LANES - span, 2) for t in tiles]
        down = [pltpu.roll(t, span, 2) for t in tiles]
        after = []
        for t in range(3):
            north = jnp.where(lane3 < LANES - span, up[t], up[min(t + 1, 2)])
            south = jnp.where(lane3 >= span, down[t], down[max(t - 1, 0)])
            v = tiles[t]
            after.append(
                0.6 * v[1:-1] + 0.025 * (v[2:] + north[1:-1]) + 0.175 * (v[:-2] + south[1:-1]))
        tiles = after
    g4[...] = tiles[1]
    forcing = (tiles[1] - g_ref[...]) * (1.0 / (0.5 * GSUB))

    rows = lax.broadcasted_iota(I32, (LANES, LANES), 0)
    cols = lax.broadcasted_iota(I32, (LANES, LANES), 1)
    flat = forcing.reshape(tile_x * fields, LANES)
    for y in range(tile_y):
        spread = jnp.where(rows == y * span + lax.div(cols, slots), 1.0, 0.0).astype(F32)
        fcol[y] = jnp.dot(flat, spread, precision=HIGH, preferred_element_type=F32).reshape(
            tile_x, fields, LANES)
    slot_of = lax.rem(lane, slots)
    for k in range(helpers):
        packed = jnp.zeros((fields, LANES), F32)
        for j in range(slots):
            c = table_ref[k * slots + j]
            v = fcol[lax.rem(c, tile_y), lax.div(c, tile_y)]
            packed = jnp.where(slot_of == j, v, packed)
        fsend[k] = packed
    fmoves = []
    for i, peer in enumerate(peers):
        fmoves.append(pltpu.make_async_remote_copy(
            src_ref=fsend.at[peer], dst_ref=frecv.at[ha],
            send_sem=f_send.at[i], recv_sem=f_recv.at[i],
            device_id={"ha": peer}, device_id_type=MESH))
        fmoves[-1].start()
    frecv[ha] = fsend[ha]

    mix = mixing_ref[...]
    mrow = lax.broadcasted_iota(I32, (fields, fields), 0)
    mcol = lax.broadcasted_iota(I32, (fields, fields), 1)
    diag = []
    for k in range(fields):
        picked = jnp.where(mcol == lax.rem(mrow + k, fields), mix, 0.0)
        diag.append(jnp.broadcast_to(
            0.1 * jnp.sum(picked, axis=1, keepdims=True), (fields, LANES)))
    chunk = max(d for d in range(1, 13) if levels_all % d == 0)

    for copy in fmoves:
        copy.wait_recv()
    even = lax.rem(lane, 2) == 0
    lane_pair = lax.div(lane, 2)
    for z in range(helpers):
        tsend[z] = jnp.zeros((fields, LANES), F32)

    for p in range(pairs):
        for z in range(helpers):
            def expand(l, carry, z=z, p=p):
                v = jnp.where(lane_pair == l * pairs + p, frecv[z], 0.0)
                push[z * levels + l] = 0.1 * pair_sum(v)
                return carry
            lax.fori_loop(0, levels, expand, 0, unroll=5 if levels % 5 == 0 else 1)
        for copy in moves[p]:
            copy.wait_recv()
        crm_ref[p] = state[p]
        first = ha * slots + 2 * p
        counts = jnp.where(even, table_ref[columns + first], table_ref[columns + first + 1])

        def one_step(k, carry, p=p, counts=counts):
            active = k < counts

            def some_levels(b, prev):
                l0 = b * chunk
                v = [prev] + [state[p, l0 + i] for i in range(chunk)]
                v.append(state[p, jnp.minimum(l0 + chunk, levels_all - 1)])
                for i in range(chunk):
                    s = v[i + 1]
                    t = jnp.tanh(s)
                    total = diag[0] * t + push[l0 + i]
                    for m in range(1, fields):
                        total = total + diag[m] * pltpu.roll(t, fields - m, 0)
                    total = total + 0.1 * (pltpu.roll(s, 2, 1) + pltpu.roll(s, LANES - 2, 1))
                    total = total + 0.05 * (v[i] + v[i + 2]) + 0.7 * s
                    state[p, l0 + i] = jnp.where(active, total, s)
                return v[chunk]

            lax.fori_loop(0, levels_all // chunk, some_levels, state[p, 0])
            return carry

        lax.fori_loop(0, MAXSUB, one_step, 0)
        for z in range(helpers):
            def finish(l, acc, z=z, p=p):
                s = state[p, z * levels + l]
                d = pair_sum(s - crm_ref[p, z * levels + l])
                crm_ref[p, z * levels + l] = s
                return jnp.where(lane_pair == l * pairs + p, d, acc)
            tsend[z] = lax.fori_loop(
                0, levels, finish, tsend[z], unroll=5 if levels % 5 == 0 else 1)

    tmoves = []
    for i, peer in enumerate(peers):
        tmoves.append(pltpu.make_async_remote_copy(
            src_ref=tsend.at[peer], dst_ref=trecv.at[ha],
            send_sem=t_send.at[i], recv_sem=t_recv.at[i],
            device_id={"ha": peer}, device_id_type=MESH))
        tmoves[-1].start()
    trecv[ha] = tsend[ha]
    for row in moves:
        for copy in row:
            copy.wait_send()
    for copy in halos + fmoves:
        copy.wait_send()
    for copy in tmoves:
        copy.wait()
    placed = jnp.zeros((tile_x * fields, LANES), F32)
    for y in range(tile_y):
        for x in range(tile_x):
            a = assign_ref[x, y]
            v = trecv[lax.div(a, slots)]
            mask[x] = jnp.where(slot_of == lax.rem(a, slots), v, 0.0)
        gather = jnp.where(
            (cols == y * span + lax.div(rows, slots)) & (rows < levels * slots), 1.0, 0.0
        ).astype(F32)
        placed = placed + jnp.dot(
            mask[...].reshape(tile_x * fields, LANES), gather,
            precision=HIGH, preferred_element_type=F32)
    newg_ref[...] = g4[...] + (1.0 / width) * placed.reshape(tile_x, fields, LANES)


def on_device(sizes, global_state, crm_state, mixing, substeps, assignment):
    n_gx, n_gy, helpers = sizes
    fields, levels = crm_state.shape[:2]
    tile_x, tile_y = assignment.shape
    width = crm_state.shape[3] // tile_y
    columns = tile_x * tile_y
    per_helper = columns // helpers
    pairs = per_helper // 2
    span = LANES // tile_y
    levels_all = levels * helpers
    assert 2 * width == LANES and tile_y == 4 and fields == 8
    assert levels * per_helper <= LANES and levels <= span
    assert tile_x >= GSUB and tile_y >= GSUB
    dims = (fields, levels, tile_x, tile_y, width, helpers, pairs)

    g = jnp.transpose(global_state, (2, 0, 3, 1))
    g = jnp.pad(g, ((0, 0), (0, 0), (0, 0), (0, span - levels))).reshape(tile_x, fields, LANES)

    smem = pl.BlockSpec(memory_space=pltpu.SMEM)
    vmem = pl.BlockSpec(memory_space=pltpu.VMEM)
    rows = fields * levels * tile_x
    flat = crm_state.reshape(rows, tile_y * width)
    slotted, table = pl.pallas_call(
        functools.partial(slot_kernel, dims),
        grid=(1,),
        out_shape=(
            jax.ShapeDtypeStruct((helpers * pairs * levels, fields, LANES), F32),
            jax.ShapeDtypeStruct((2 * columns,), I32),
        ),
        in_specs=[
            smem, smem,
            pl.BlockSpec((rows, LANES), lambda i: (0, 0)),
            pl.BlockSpec((rows, LANES), lambda i: (0, 1)),
        ],
        out_specs=(
            pl.BlockSpec((helpers * pairs * levels, fields, LANES), lambda i: (0, 0, 0)), smem),
    )(assignment, substeps, flat, flat)

    dma = pltpu.SemaphoreType.DMA
    vec = (fields, LANES)
    peers = helpers - 1
    crm, newg = pl.pallas_call(
        functools.partial(exchange_kernel, dims, (n_gx, n_gy)),
        out_shape=(
            jax.ShapeDtypeStruct((pairs, levels_all) + vec, F32),
            jax.ShapeDtypeStruct((tile_x,) + vec, F32),
        ),
        in_specs=[smem, smem, vmem, vmem, vmem],
        out_specs=(vmem, vmem),
        scratch_shapes=[
            pltpu.VMEM((pairs, levels_all) + vec, F32),
            pltpu.VMEM((levels_all,) + vec, F32),
            pltpu.VMEM((3, tile_x + 2 * GSUB) + vec, F32),
            pltpu.VMEM((tile_x,) + vec, F32),
            pltpu.VMEM((tile_y, tile_x) + vec, F32),
            pltpu.VMEM((helpers,) + vec, F32),
            pltpu.VMEM((helpers,) + vec, F32),
            pltpu.VMEM((helpers,) + vec, F32),
            pltpu.VMEM((helpers,) + vec, F32),
            pltpu.VMEM((tile_x,) + vec, F32),
            dma((8,)), dma((8,)),
            dma((pairs, peers)), dma((pairs, peers)),
            dma((peers,)), dma((peers,)),
            dma((peers,)), dma((peers,)),
        ],
        compiler_params=pltpu.CompilerParams(collective_id=0, has_side_effects=True),
    )(assignment, table, slotted, g, mixing)

    new_crm = pl.pallas_call(
        functools.partial(order_kernel, (fields, levels_all, width)),
        grid=(pairs,),
        out_shape=jax.ShapeDtypeStruct((fields, levels_all, per_helper * width), F32),
        in_specs=[pl.BlockSpec((levels_all * fields, LANES), lambda p: (p, 0))],
        out_specs=pl.BlockSpec((fields, levels_all, LANES), lambda p: (0, 0, p)),
    )(crm.reshape(pairs * levels_all * fields, LANES))

    newg = newg.reshape(tile_x, fields, tile_y, span)[..., :levels]
    return jnp.transpose(newg, (1, 3, 0, 2)), new_crm


def solution(mesh):
    sizes = (mesh.shape["gx"], mesh.shape["gy"], mesh.shape["ha"])
    in_specs = (
        P(None, "ha", "gx", "gy"),
        P(None, "ha", "gx", "gy"),
        P(),
        P("gx", "gy"),
        P("gx", "gy"),
    )
    out_specs = (P(None, "ha", "gx", "gy"), P(None, None, ("gx", "gy", "ha")))
    return jax.shard_map(
        functools.partial(on_device, sizes),
        mesh=mesh, in_specs=in_specs, out_specs=out_specs, check_vma=False,
    )
```

```python
import functools

import jax
import jax.numpy as jnp
from jax import lax
from jax.experimental import pallas as pl
from jax.experimental.pallas import tpu as pltpu
from jax.sharding import PartitionSpec as P

MAXSUB = 8
GSUB = 4
LANES = 128
CHUNK = 20
MESH = pl.DeviceIdType.MESH
HIGH = lax.Precision.HIGHEST
F32 = jnp.float32
I32 = jnp.int32


def lane_iota(shape):
    return lax.broadcasted_iota(I32, shape, len(shape) - 1)


def slot_kernel(dims, assign_ref, steps_ref, low_ref, high_ref, slots_ref, table_ref):
    fields, levels, tile_x, tile_y, width, helpers, pairs = dims
    columns = tile_x * tile_y
    for x in range(tile_x):
        for y in range(tile_y):
            v = assign_ref[y, x]
            table_ref[v] = x * tile_y + y
            table_ref[columns + v] = steps_ref[y, x]
    lane = lane_iota((fields, LANES))
    even = lax.rem(lane, 2) == 0
    half = lax.div(lane, 2)

    def one_pair(q, carry):
        ca = table_ref[2 * q]
        cb = table_ref[2 * q + 1]
        xa, ya = lax.div(ca, tile_y), lax.rem(ca, tile_y)
        xb, yb = lax.div(cb, tile_y), lax.rem(cb, tile_y)
        ia = half + lax.rem(ya, 2) * width
        ib = half + lax.rem(yb, 2) * width
        ta, tb = ya < 2, yb < 2
        for l in range(levels):
            rows_a = pl.ds(l * tile_x + xa, fields, stride=levels * tile_x)
            rows_b = pl.ds(l * tile_x + xb, fields, stride=levels * tile_x)
            a = jnp.where(ta, low_ref[rows_a, :], high_ref[rows_a, :])
            b = jnp.where(tb, low_ref[rows_b, :], high_ref[rows_b, :])
            a = jnp.take_along_axis(a, ia, axis=1)
            b = jnp.take_along_axis(b, ib, axis=1)
            slots_ref[q * levels + l] = jnp.where(even, a, b)
        return carry

    lax.fori_loop(0, helpers * pairs, one_pair, 0)


def order_kernel(dims, in_ref, out_ref):
    levels_all, width = dims
    lane = lane_iota(in_ref.shape[1:])
    index = 2 * lax.rem(lane, width) + lax.div(lane, width)
    for l in range(levels_all):
        out_ref[l] = jnp.take_along_axis(in_ref[l], index, axis=1)


def expand_levels(v, lane, slots, p):
    v = jnp.where(lax.div(lax.rem(lane, slots), 2) == p, v, 0.0)
    if p > 0:
        v = pltpu.roll(v, LANES - 2 * p, 1)
    shift = 2
    while shift < slots:
        v = v + pltpu.roll(v, shift, 1)
        shift *= 2
    parts = [v]
    while shift < LANES:
        clear = (lane & shift) == 0
        low = [jnp.where(clear, u, pltpu.roll(u, shift, 1)) for u in parts]
        high = [jnp.where(clear, pltpu.roll(u, LANES - shift, 1), u) for u in parts]
        parts = low + high
        shift *= 2
    return parts


def fold_levels(parts, lane, slots):
    shift = LANES // 2
    while shift >= slots:
        clear = (lane & shift) == 0
        half = len(parts) // 2
        after = []
        for a, b in zip(parts[:half], parts[half:]):
            after.append(jnp.where(
                clear, a + pltpu.roll(a, LANES - shift, 1), b + pltpu.roll(b, shift, 1)))
        parts = after
        shift //= 2
    v = parts[0]
    while shift >= 2:
        v = v + jnp.where(
            (lane & shift) == 0, pltpu.roll(v, LANES - shift, 1), pltpu.roll(v, shift, 1))
        shift //= 2
    return v


def exchange_kernel(
    dims, sizes, assign_ref, table_ref, slots_ref, g_ref, mixing_ref, crm_ref, newg_ref,
    state, push, ext, diag, g4, fcol, fsend, frecv, tsend, trecv, mask,
    halo_send, halo_recv, crm_send, crm_recv, f_send, f_recv, t_send, t_recv,
):
    fields, levels, tile_x, tile_y, width, helpers, pairs = dims
    n_gx, n_gy = sizes
    columns = tile_x * tile_y
    levels_all = levels * helpers
    slots = 2 * pairs
    span = LANES // tile_y
    h = GSUB
    gx, gy, ha = lax.axis_index("gx"), lax.axis_index("gy"), lax.axis_index("ha")

    offsets = [(dx, dy) for dx in (0, 1, -1) for dy in (0, 1, -1) if (dx, dy) != (0, 0)]

    def tile_at(dx, dy):
        return {"gx": lax.rem(gx + dx + n_gx, n_gx), "gy": lax.rem(gy + dy + n_gy, n_gy)}

    peers = [lax.rem(ha + i, helpers) for i in range(1, helpers)]
    barrier = pltpu.get_barrier_semaphore()
    for dx, dy in offsets:
        pl.semaphore_signal(barrier, inc=1, device_id=tile_at(dx, dy), device_id_type=MESH)
    for peer in peers:
        pl.semaphore_signal(barrier, inc=1, device_id={"ha": peer}, device_id_type=MESH)
    pl.semaphore_wait(barrier, len(offsets) + len(peers))

    halos = []
    for o, (dx, dy) in enumerate(offsets):
        if dx == 0:
            src, dst = g_ref, ext.at[1 - dy, pl.ds(h, tile_x)]
        elif dx == 1:
            src, dst = g_ref.at[pl.ds(tile_x - h, h)], ext.at[1 - dy, pl.ds(0, h)]
        else:
            src, dst = g_ref.at[pl.ds(0, h)], ext.at[1 - dy, pl.ds(tile_x + h, h)]
        halos.append(pltpu.make_async_remote_copy(
            src_ref=src, dst_ref=dst, send_sem=halo_send.at[o], recv_sem=halo_recv.at[o],
            device_id=tile_at(dx, dy), device_id_type=MESH))
        halos[-1].start()
    moves = []
    for p in range(pairs):
        row = []
        for i, peer in enumerate(peers):
            row.append(pltpu.make_async_remote_copy(
                src_ref=slots_ref.at[pl.ds((peer * pairs + p) * levels, levels)],
                dst_ref=state.at[p, pl.ds(ha * levels, levels)],
                send_sem=crm_send.at[p, i], recv_sem=crm_recv.at[p, i],
                device_id={"ha": peer}, device_id_type=MESH))
            row[-1].start()
        moves.append(row)

    for p in range(pairs):
        for l in range(levels):
            state[p, ha * levels + l] = slots_ref[(ha * pairs + p) * levels + l]
    ext[1, h:h + tile_x] = g_ref[...]
    lane = lane_iota((fields, LANES))
    lane3 = lane_iota((1, 1, LANES))
    for copy in halos:
        copy.wait_recv()
    tiles = [ext[t] for t in range(3)]
    for _ in range(GSUB):
        up = [pltpu.roll(t, LANES - span, 2) for t in tiles]
        down = [pltpu.roll(t, span, 2) for t in tiles]
        after = []
        for t in range(3):
            north = jnp.where(lane3 < LANES - span, up[t], up[min(t + 1, 2)])
            south = jnp.where(lane3 >= span, down[t], down[max(t - 1, 0)])
            v = tiles[t]
            after.append(
                0.6 * v[1:-1] + 0.025 * (v[2:] + north[1:-1]) + 0.175 * (v[:-2] + south[1:-1]))
        tiles = after
    g4[...] = tiles[1]
    forcing = (tiles[1] - g_ref[...]) * (1.0 / (0.5 * GSUB))

    rows = lax.broadcasted_iota(I32, (LANES, LANES), 0)
    cols = lax.broadcasted_iota(I32, (LANES, LANES), 1)
    flat = forcing.reshape(tile_x * fields, LANES)
    for y in range(tile_y):
        spread = jnp.where(rows == y * span + lax.div(cols, slots), 1.0, 0.0).astype(F32)
        fcol[y] = jnp.dot(flat, spread, precision=HIGH, preferred_element_type=F32).reshape(
            tile_x, fields, LANES)
    slot_of = lax.rem(lane, slots)
    for k in range(helpers):
        packed = jnp.zeros((fields, LANES), F32)
        for j in range(slots):
            c = table_ref[k * slots + j]
            v = fcol[lax.rem(c, tile_y), lax.div(c, tile_y)]
            packed = jnp.where(slot_of == j, v, packed)
        fsend[k] = packed
    fmoves = []
    for i, peer in enumerate(peers):
        fmoves.append(pltpu.make_async_remote_copy(
            src_ref=fsend.at[peer], dst_ref=frecv.at[ha],
            send_sem=f_send.at[i], recv_sem=f_recv.at[i],
            device_id={"ha": peer}, device_id_type=MESH))
        fmoves[-1].start()
    frecv[ha] = fsend[ha]

    mix = mixing_ref[...]
    mrow = lax.broadcasted_iota(I32, (fields, fields), 0)
    mcol = lax.broadcasted_iota(I32, (fields, fields), 1)
    for k in range(fields):
        picked = jnp.where(mcol == lax.rem(mrow + k, fields), mix, 0.0)
        diag[k] = jnp.broadcast_to(
            0.1 * jnp.sum(picked, axis=1, keepdims=True), (fields, LANES))
    chunk = max(d for d in range(1, CHUNK + 1) if levels_all % d == 0)

    for copy in fmoves:
        copy.wait_recv()
    even = lax.rem(lane, 2) == 0
    pair_of = lax.div(lax.rem(lane, slots), 2)
    for p in range(pairs):
        for z in range(helpers):
            parts = expand_levels(0.1 * frecv[z], lane, slots, p)
            for l in range(levels):
                push[p, z * levels + l] = parts[l]

    sums = [jnp.zeros((fields, LANES), F32)] * helpers
    for p in range(pairs):
        for copy in moves[p]:
            copy.wait_recv()
        first = ha * slots + 2 * p
        counts = jnp.where(even, table_ref[columns + first], table_ref[columns + first + 1])

        def one_step(k, source, p=p, counts=counts):
            active = k < counts

            def some_levels(b, prev):
                l0 = b * chunk
                v = [prev] + [source[p, l0 + i] for i in range(chunk)]
                v.append(source[p, jnp.minimum(l0 + chunk, levels_all - 1)])
                for i in range(chunk):
                    s = v[i + 1]
                    t = jnp.tanh(s)
                    total = diag[0] * t + push[p, l0 + i]
                    for m in range(1, fields):
                        total = total + diag[m] * pltpu.roll(t, fields - m, 0)
                    total = total + 0.1 * (pltpu.roll(s, 2, 1) + pltpu.roll(s, LANES - 2, 1))
                    total = total + 0.05 * (v[i] + v[i + 2]) + 0.7 * s
                    crm_ref[p, l0 + i] = jnp.where(active, total, s)
                return v[chunk]

            lax.fori_loop(0, levels_all // chunk, some_levels, source[p, 0])

        def later_step(k, carry):
            one_step(k, crm_ref)
            return carry

        one_step(0, state)
        lax.fori_loop(1, MAXSUB, later_step, 0)
        zero = jnp.zeros((fields, LANES), F32)
        for z in range(helpers):
            parts = [crm_ref[p, z * levels + l] - state[p, z * levels + l] for l in range(levels)]
            parts += [zero] * (LANES // slots - levels)
            sums[z] = jnp.where(pair_of == p, fold_levels(parts, lane, slots), sums[z])

    for z in range(helpers):
        tsend[z] = sums[z]
    tmoves = []
    for i, peer in enumerate(peers):
        tmoves.append(pltpu.make_async_remote_copy(
            src_ref=tsend.at[peer], dst_ref=trecv.at[ha],
            send_sem=t_send.at[i], recv_sem=t_recv.at[i],
            device_id={"ha": peer}, device_id_type=MESH))
        tmoves[-1].start()
    trecv[ha] = tsend[ha]
    for row in moves:
        for copy in row:
            copy.wait_send()
    for copy in halos + fmoves:
        copy.wait_send()
    for copy in tmoves:
        copy.wait()
    placed = jnp.zeros((tile_x * fields, LANES), F32)
    for y in range(tile_y):
        for x in range(tile_x):
            a = assign_ref[y, x]
            v = trecv[lax.div(a, slots)]
            mask[x] = jnp.where(slot_of == lax.rem(a, slots), v, 0.0)
        gather = jnp.where(
            (cols == y * span + lax.div(rows, slots)) & (rows < levels * slots), 1.0, 0.0
        ).astype(F32)
        placed = placed + jnp.dot(
            mask[...].reshape(tile_x * fields, LANES), gather,
            precision=HIGH, preferred_element_type=F32)
    newg_ref[...] = g4[...] + (1.0 / width) * placed.reshape(tile_x, fields, LANES)


def on_device(sizes, global_state, crm_state, mixing, substeps, assignment):
    n_gx, n_gy, helpers = sizes
    fields, levels = crm_state.shape[:2]
    tile_x, tile_y = assignment.shape
    width = crm_state.shape[3] // tile_y
    columns = tile_x * tile_y
    per_helper = columns // helpers
    pairs = per_helper // 2
    span = LANES // tile_y
    levels_all = levels * helpers
    assert 2 * width == LANES and tile_y == 4 and fields == 8
    assert LANES % per_helper == 0 and levels <= LANES // per_helper and levels <= span
    assert tile_x >= GSUB and tile_y >= GSUB
    dims = (fields, levels, tile_x, tile_y, width, helpers, pairs)

    g = jnp.transpose(global_state, (2, 0, 3, 1))
    g = jnp.pad(g, ((0, 0), (0, 0), (0, 0), (0, span - levels))).reshape(tile_x, fields, LANES)

    smem = pl.BlockSpec(memory_space=pltpu.SMEM)
    vmem = pl.BlockSpec(memory_space=pltpu.VMEM)
    rows = fields * levels * tile_x
    flat = crm_state.reshape(rows, tile_y * width)
    slotted, table = pl.pallas_call(
        functools.partial(slot_kernel, dims),
        grid=(1,),
        out_shape=(
            jax.ShapeDtypeStruct((helpers * pairs * levels, fields, LANES), F32),
            jax.ShapeDtypeStruct((2 * columns,), I32),
        ),
        in_specs=[
            smem, smem,
            pl.BlockSpec((rows, LANES), lambda i: (0, 0)),
            pl.BlockSpec((rows, LANES), lambda i: (0, 1)),
        ],
        out_specs=(
            pl.BlockSpec((helpers * pairs * levels, fields, LANES), lambda i: (0, 0, 0)), smem),
    )(assignment.T, substeps.T, flat, flat)

    dma = pltpu.SemaphoreType.DMA
    vec = (fields, LANES)
    peers = helpers - 1
    crm, newg = pl.pallas_call(
        functools.partial(exchange_kernel, dims, (n_gx, n_gy)),
        out_shape=(
            jax.ShapeDtypeStruct((pairs, levels_all) + vec, F32),
            jax.ShapeDtypeStruct((tile_x,) + vec, F32),
        ),
        in_specs=[smem, smem, vmem, vmem, vmem],
        out_specs=(vmem, vmem),
        scratch_shapes=[
            pltpu.VMEM((pairs, levels_all) + vec, F32),
            pltpu.VMEM((pairs, levels_all) + vec, F32),
            pltpu.VMEM((3, tile_x + 2 * GSUB) + vec, F32),
            pltpu.VMEM((fields,) + vec, F32),
            pltpu.VMEM((tile_x,) + vec, F32),
            pltpu.VMEM((tile_y, tile_x) + vec, F32),
            pltpu.VMEM((helpers,) + vec, F32),
            pltpu.VMEM((helpers,) + vec, F32),
            pltpu.VMEM((helpers,) + vec, F32),
            pltpu.VMEM((helpers,) + vec, F32),
            pltpu.VMEM((tile_x,) + vec, F32),
            dma((8,)), dma((8,)),
            dma((pairs, peers)), dma((pairs, peers)),
            dma((peers,)), dma((peers,)),
            dma((peers,)), dma((peers,)),
        ],
        compiler_params=pltpu.CompilerParams(collective_id=0, has_side_effects=True),
    )(assignment.T, table, slotted, g, mixing)

    new_crm = pl.pallas_call(
        functools.partial(order_kernel, (levels_all, width)),
        grid=(pairs,),
        out_shape=jax.ShapeDtypeStruct((levels_all, fields, per_helper * width), F32),
        in_specs=[pl.BlockSpec((levels_all, fields, LANES), lambda p: (p, 0, 0))],
        out_specs=pl.BlockSpec((levels_all, fields, LANES), lambda p: (0, 0, p)),
    )(crm.reshape(pairs * levels_all, fields, LANES))

    newg = newg.reshape(tile_x, fields, tile_y, span)[..., :levels]
    return jnp.transpose(newg, (1, 3, 0, 2)), jnp.transpose(new_crm, (1, 0, 2))


def solution(mesh):
    sizes = (mesh.shape["gx"], mesh.shape["gy"], mesh.shape["ha"])
    in_specs = (
        P(None, "ha", "gx", "gy"),
        P(None, "ha", "gx", "gy"),
        P(),
        P("gx", "gy"),
        P("gx", "gy"),
    )
    out_specs = (P(None, "ha", "gx", "gy"), P(None, None, ("gx", "gy", "ha")))
    return jax.shard_map(
        functools.partial(on_device, sizes),
        mesh=mesh, in_specs=in_specs, out_specs=out_specs, check_vma=False,
    )
```
